32 devices in a mesh: row: 8 (over y, x, core), col: 4 (over z).
Axes of the slice: x: 2, y: 2, z: 4, core: 2. Of those that a mesh axis runs over, the one named last changes fastest.
Arguments:
- a_window: float32 [16384, 4096], P('row', 'col'), may hold values from -6 to 6
- l_panel: float32 [16384, 1024], P('row'), may hold values from -0.1875 to 0.1875
- l_inverse: float32 [2, 512, 512], replicated, may hold values from -2 to 2, as said below
Outputs:
- reduced: float32 [16384, 4096], P('row', 'col')
The draws below stay inside these ranges and needn't reach their ends.
Inputs may be any that keep to these rules, and one draw needn't show every extreme that they name: `l_inverse`: both blocks are lower triangular, with diagonal entries between 0.5 and 2.
All inputs are finite; a program needn't handle non-finite values.
Results may differ from the reference program's by a relative error of at most 0.000067.
Values sent between devices are 32-bit elements; how exact they have to be, the bound alone decides.
A program may use at most 128 MiB of HBM per device.

```python
import jax
import jax.numpy as jnp
from jax import lax

N = 16384
B = 512
WC = 4096


def draw_l_inverse(key, part):
    first_key, second_key = jax.random.split(jax.random.fold_in(key, 17))
    spread = jnp.clip(jax.random.normal(first_key, (2, B, B), jnp.float32), -4.0, 4.0)
    diagonal = jax.random.uniform(second_key, (2, B), jnp.float32, 0.5, 1.5)
    strict = jnp.tril(spread, -1) / jnp.sqrt(jnp.float32(B))
    return strict + diagonal[:, :, None] * jnp.eye(B, dtype=jnp.float32)[None, :, :]


def shard_levels(own_key, extent, pieces, least, top_value):
    level, own = 1.0, jax.random.fold_in(own_key, 6)
    for axis_at, shards_of in pieces:
        steps = jnp.exp(jax.random.uniform(jax.random.fold_in(own, axis_at), (shards_of,), jnp.float32, least / len(pieces), top_value / len(pieces)))
        level = level * jnp.repeat(steps, extent[axis_at] // shards_of).reshape([-1 if axis == axis_at else 1 for axis in range(len(extent))])
    return level


def noise(own_key, shape, deviation, reach, cuts=(), kind=jnp.bfloat16):
    loudness = shard_levels(own_key, shape, cuts, -0.22, 0.18) if cuts else 1.0
    drawn = jax.random.normal(own_key, shape, jnp.float32) * deviation * loudness
    return jnp.minimum(jnp.maximum(drawn, -reach), reach).astype(kind)


def setup_inputs(seed: int = 0) -> dict:
    key_list = jax.random.split(jax.random.key(seed), 4)
    a_window = noise(key_list[0], (N, WC), 1.0, 6.0, ((0, 8), (1, 4)), jnp.float32)
    l_panel = noise(key_list[1], (N, 2 * B), (2 * B) ** -0.5, 0.1875, ((0, 8),), jnp.float32)
    l_inverse = draw_l_inverse(jax.random.fold_in(key_list[3], 71), 0)
    return {"a_window": a_window, "l_panel": l_panel, "l_inverse": l_inverse}


def matmul_hp(left, right):
    return jnp.dot(left, right, precision=lax.Precision.HIGHEST, preferred_element_type=jnp.float32)


def reference(a_window, l_panel, l_inverse):
    first_inv = l_inverse[0]
    second_inv = l_inverse[1]
    coupling = l_panel[B:2 * B, :B]
    leading = matmul_hp(a_window[:, :B], first_inv.T)
    second_col = matmul_hp(a_window[:, B:2 * B] - matmul_hp(leading, coupling.T), second_inv.T)
    solved = jnp.concatenate([leading, second_col], 1)
    upper_tile = matmul_hp(first_inv, solved[:B])
    lower_tile = matmul_hp(second_inv, solved[B:2 * B] - matmul_hp(coupling, upper_tile))
    diag_block = jnp.concatenate([upper_tile, lower_tile], 0)
    below = l_panel[2 * B:]
    product = matmul_hp(below, diag_block)
    reduced_g = solved[2 * B:] - 0.5 * product
    lower_panel = solved[2 * B:] - product
    width_left = WC - 2 * B
    update = a_window[2 * B:, 2 * B:] - matmul_hp(below, reduced_g[:width_left].T) - matmul_hp(reduced_g, below[:width_left].T)
    upper_rows = jnp.concatenate([diag_block, a_window[:2 * B, 2 * B:]], 1)
    lower_rows = jnp.concatenate([lower_panel, update], 1)
    return jnp.concatenate([upper_rows, lower_rows], 0)
```

```python
import functools

import jax
import jax.numpy as jnp
from jax import lax
from jax.experimental import pallas as pl
from jax.experimental.pallas import tpu as pltpu
from jax.sharding import PartitionSpec as P

MESH = pl.DeviceIdType.MESH
STEPS = 16


def bits_of(count):
    return max(count.bit_length() - 1, 0)


def ring_pos(index, count):
    if count & (count - 1):
        return index
    parity, place = 0, 0
    for bit in reversed(range(bits_of(count))):
        parity = (parity + (index // 2**bit) % 2) % 2
        place = place + parity * 2**bit
    return place


def ring_at(place, count):
    if count & (count - 1):
        return place
    index = 0
    for bit in range(bits_of(count)):
        index = index + (((place // 2**bit) % 2 + (place // 2 ** (bit + 1)) % 2) % 2) * 2**bit
    return index


def move_kernel(
    rows_n, cols_n, width, half, a_ref, l_ref, rows_ref, top_ref, tile_ref, lower_ref, couple_ref, zs, zr, rs, rr
):
    row, col = lax.axis_index("row"), lax.axis_index("col")
    depth = a_ref.shape[0]
    blocks = depth // width
    chunk = width // 2 // STEPS
    z_steps = blocks * STEPS
    span = depth // z_steps
    place = ring_pos(row, rows_n)
    root = (col * width) // depth
    root_place = ring_pos(root, rows_n)
    offset = (col * width) % depth
    z_next = (col + 1) % cols_n
    z_last = (col + cols_n - 1) % cols_n
    r_next = (ring_at((place + 1) % rows_n, rows_n), ring_at((place + rows_n - 1) % rows_n, rows_n))

    barrier = pltpu.get_barrier_semaphore()
    for other in (z_next, z_last):
        pl.semaphore_signal(barrier, inc=1, device_id=(row, other), device_id_type=MESH)
    for other in r_next:
        pl.semaphore_signal(barrier, inc=1, device_id=(other, col), device_id_type=MESH)
    pl.semaphore_wait(barrier, 4)

    def z_copy(step, source):
        at = step * span
        return pltpu.make_async_remote_copy(
            src_ref=source.at[pl.ds(at, span)],
            dst_ref=rows_ref.at[pl.ds(at, span)],
            send_sem=zs.at[step],
            recv_sem=zr.at[step],
            device_id=(row, z_next),
            device_id_type=MESH,
        )

    z_sends = col != cols_n - 1

    def z_step(step):
        @pl.when(col == 0)
        def _():
            z_copy(step, a_ref).start()

        @pl.when(col != 0)
        def _():
            z_copy(step, rows_ref).wait_recv()

            @pl.when(z_sends)
            def _():
                z_copy(step, rows_ref).start()

    small = half // 2 // STEPS
    items = (
        (couple_ref, small, half // 2, 0),
        (lower_ref, chunk, width // 2, root_place),
        (top_ref, chunk, width // 2, 0),
        (tile_ref, chunk, width // 2, root_place),
    )

    def distance(item, way):
        start = items[item][3]
        return (place - start + rows_n) % rows_n if way == 0 else (start - place + rows_n) % rows_n

    def r_copy(item, way, step, source, shift, columns=None):
        buffer, count, part, _ = items[item]
        at = (2 * step + way) * count
        view = source.at[pl.ds(shift + at, count)] if columns is None else source.at[pl.ds(shift + at, count), columns]
        return pltpu.make_async_remote_copy(
            src_ref=view,
            dst_ref=buffer.at[pl.ds(at, count)],
            send_sem=rs.at[item, way, step],
            recv_sem=rr.at[item, way, step],
            device_id=(r_next[way], col),
            device_id_type=MESH,
        )

    def r_step(item, way, step):
        far = distance(item, way)

        @pl.when(far == 0)
        def _():
            if item == 0:
                r_copy(item, way, step, l_ref, half, pl.ds(0, half)).start()
            elif item == 1:
                r_copy(item, way, step, l_ref, offset).start()
            elif item == 2:
                @pl.when(col == 0)
                def _():
                    r_copy(item, way, step, a_ref, 0).start()

                @pl.when(col != 0)
                def _():
                    r_copy(item, way, step, rows_ref, 0).start()
            else:
                r_copy(item, way, step, rows_ref, offset).start()

        @pl.when(far != 0)
        def _():
            r_copy(item, way, step, items[item][0], 0).wait_recv()

            @pl.when(far != rows_n - 1)
            def _():
                r_copy(item, way, step, items[item][0], 0).start()

    def wanted(item):
        return col != 0 if item in (1, 3) else col >= 0

    first = (0, 0, 0, z_steps - STEPS)

    @pl.loop(0, z_steps + rows_n - 1)
    def _(i):
        @pl.when(i < z_steps)
        def _():
            z_step(i)

        for item in range(4):
            for way in range(2):
                step = i - distance(item, way) - first[item]

                @pl.when(jnp.logical_and(wanted(item), jnp.logical_and(step >= 0, step < STEPS)))
                def _():
                    r_step(item, way, step)

    @pl.loop(0, z_steps)
    def _(i):
        @pl.when(z_sends)
        def _():
            z_copy(i, rows_ref).wait_send()

    @pl.loop(0, STEPS)
    def _(i):
        for item in range(4):
            for way in range(2):
                @pl.when(jnp.logical_and(wanted(item), distance(item, way) != rows_n - 1))
                def _():
                    r_copy(item, way, i, items[item][0], 0).wait_send()


def move(rows_n, cols_n, width, half, a_window, l_panel):
    depth = a_window.shape[0]
    f32 = jnp.float32
    square = jax.ShapeDtypeStruct((width, width), f32)
    z_steps = depth // width * STEPS
    return pl.pallas_call(
        functools.partial(move_kernel, rows_n, cols_n, width, half),
        out_shape=(
            jax.ShapeDtypeStruct((depth, width), f32),
            square,
            square,
            square,
            jax.ShapeDtypeStruct((half, half), f32),
        ),
        in_specs=[pl.BlockSpec(memory_space=pl.ANY)] * 2,
        out_specs=[pl.BlockSpec(memory_space=pl.ANY)] * 5,
        scratch_shapes=[
            pltpu.SemaphoreType.DMA((z_steps,)),
            pltpu.SemaphoreType.DMA((z_steps,)),
            pltpu.SemaphoreType.DMA((4, 2, STEPS)),
            pltpu.SemaphoreType.DMA((4, 2, STEPS)),
        ],
        compiler_params=pltpu.CompilerParams(collective_id=0, has_side_effects=True),
    )(a_window, l_panel)


def dot(left, right, dims=((1,), (0,)), precision=lax.Precision.HIGH):
    return lax.dot_general(left, right, (dims, ((), ())), precision=precision, preferred_element_type=jnp.float32)


def split(value):
    high = value.astype(jnp.bfloat16)
    return high, (value - high.astype(jnp.float32)).astype(jnp.bfloat16)


def three_pass(left, high, low, dims):
    left_high, left_low = split(left)
    total = lax.dot_general(left_high, high, (dims, ((), ())), preferred_element_type=jnp.float32)
    total += lax.dot_general(left_high, low, (dims, ((), ())), preferred_element_type=jnp.float32)
    return total + lax.dot_general(left_low, high, (dims, ((), ())), preferred_element_type=jnp.float32)


def prepare_kernel(
    width, flags, low_own, low_got, tile_own, tile_got, a_ref, moved_ref, top_ref, inv_ref, key_ref, weight_ref, th, tl, ih, il
):
    at = pl.program_id(0)
    count = low_own.shape[0]
    in_panel, first_row, here = flags[0] == 1, flags[1] == 1, flags[2] == 1
    nn, nt = ((1,), (0,)), ((1,), (1,))

    @pl.when(at == 0)
    def _():
        @pl.loop(0, width // 128)
        def _(i):
            rows = pl.ds(i * 128, 128)
            own = jnp.where(in_panel, a_ref[rows], moved_ref[rows])
            th[rows], tl[rows] = split(jnp.where(first_row, own, top_ref[rows]))
            ih[rows], il[rows] = split(inv_ref[rows])

    lower = jnp.where(here, low_own[...], low_got[...])
    tile = jnp.where(here, tile_own[...], tile_got[...])
    inverse = inv_ref[pl.ds(pl.multiple_of(at * count, count), count)]
    scaled = three_pass(lower, ih[...], il[...], nn)
    left = jnp.where(in_panel, inverse, -0.5 * scaled)
    other = jnp.where(in_panel, 0.0, left)
    total = three_pass(left, th[...], tl[...], nt) + three_pass(other, th[...], tl[...], nn)
    weight_ref[...] = jnp.where(in_panel, 0.0, tile) + total
    key_ref[...] = jnp.where(in_panel, -inverse, scaled)


def prepare(flags, a_window, moved, l_panel, top, tile, lower, inverse):
    width = a_window.shape[1]
    count = min(256, width)
    own = pl.BlockSpec((count, width), lambda i, f: (f[3] * (width // count) + i, 0))
    block = pl.BlockSpec((count, width), lambda i, f: (i, 0))
    whole = pl.BlockSpec((width, width), lambda i, f: (0, 0))
    square = jax.ShapeDtypeStruct((width, width), jnp.float32)
    return pl.pallas_call(
        functools.partial(prepare_kernel, width),
        out_shape=(square, square),
        grid_spec=pltpu.PrefetchScalarGridSpec(
            num_scalar_prefetch=1,
            grid=(width // count,),
            in_specs=[own, block, own, block, whole, whole, whole, whole],
            out_specs=[block, block],
            scratch_shapes=[pltpu.VMEM((width, width), jnp.bfloat16)] * 4,
        ),
        compiler_params=pltpu.CompilerParams(
            dimension_semantics=("arbitrary",), vmem_limit_bytes=60 * 1024 * 1024
        ),
    )(flags, l_panel, lower, moved, tile, a_window, moved, top, inverse)


def update_kernel(
    width, flags, a_ref, moved_ref, l_ref, inv_ref, key_ref, weight_ref, out_ref, ih, il, kh, kl, wh, wl
):
    at = pl.program_id(0)
    count = a_ref.shape[0]
    half = width // 2

    @pl.when(at == 0)
    def _():
        for source, high, low in ((inv_ref, ih, il), (key_ref, kh, kl), (weight_ref, wh, wl)):
            @pl.loop(0, width // 128)
            def _(i):
                rows = pl.ds(i * 128, 128)
                high[rows], low[rows] = split(source[rows])

    in_panel = flags[0] == 1
    is_top = jnp.logical_and(flags[1] == 1, at * count < width)
    lower = l_ref[...]
    nn, nt = ((1,), (0,)), ((1,), (1,))
    scaled = jnp.concatenate(
        [
            three_pass(lower, ih[:, :half], il[:, :half], nn),
            three_pass(lower[:, half:], ih[half:, half:], il[half:, half:], nn),
        ],
        1,
    )
    own = inv_ref[pl.ds(pl.multiple_of((at * count) % width, count), count)]
    fill = jnp.where(in_panel, -own, 0.0)
    scaled = jnp.where(is_top, fill, scaled)
    window = a_ref[...]
    left = jnp.where(is_top, 0.0, jnp.where(in_panel, window, moved_ref[...]))
    base = jnp.where(in_panel, 0.0, window)
    total = three_pass(left, kh[...], kl[...], nt)
    out_ref[...] = base - (total + three_pass(scaled, wh[...], wl[...], nt))


def update(flags, a_window, moved, l_panel, inverse, key, weight):
    depth, width = a_window.shape
    count = min(256, width)
    block = pl.BlockSpec((count, width), lambda i, f: (i, 0))
    whole = pl.BlockSpec((width, width), lambda i, f: (0, 0))
    return pl.pallas_call(
        functools.partial(update_kernel, width),
        out_shape=jax.ShapeDtypeStruct((depth, width), jnp.float32),
        grid_spec=pltpu.PrefetchScalarGridSpec(
            num_scalar_prefetch=1,
            grid=(depth // count,),
            in_specs=[block, block, block, whole, whole, whole],
            out_specs=block,
            scratch_shapes=[pltpu.VMEM((width, width), jnp.bfloat16)] * 6,
        ),
        compiler_params=pltpu.CompilerParams(
            dimension_semantics=("arbitrary",), vmem_limit_bytes=60 * 1024 * 1024
        ),
    )(flags, a_window, moved, l_panel, inverse, key, weight)


def body(rows_n, cols_n, a_window, l_panel, l_inverse):
    depth, width = a_window.shape
    half = l_inverse.shape[1]
    row, col = lax.axis_index("row"), lax.axis_index("col")
    root, offset = (col * width) // depth, (col * width) % depth
    first_inv, second_inv = l_inverse[0], l_inverse[1]
    moved, top, tile, lower, couple = move(rows_n, cols_n, width, half, a_window, l_panel)
    in_panel = col == 0
    couple = jnp.where(row == 0, l_panel[half:width, :half], couple)

    full = lax.Precision.HIGHEST
    corner = -dot(second_inv, dot(couple, first_inv, precision=full), precision=full)
    inverse = jnp.concatenate(
        [jnp.concatenate([first_inv, jnp.zeros_like(first_inv)], 1), jnp.concatenate([corner, second_inv], 1)], 0
    )
    flags = jnp.stack([jnp.int32(in_panel), jnp.int32(row == 0), jnp.int32(row == root), offset // width])
    key, weight = prepare(flags, a_window, moved, l_panel, top, tile, lower, inverse)
    return update(flags, a_window, moved, l_panel, inverse, key, weight)


def solution(mesh):
    placed = (P("row", "col"), P("row", None), P())
    return jax.shard_map(
        functools.partial(body, mesh.shape["row"], mesh.shape["col"]),
        mesh=mesh,
        in_specs=placed,
        out_specs=P("row", "col"),
        check_vma=False,
    )
```
